32 devices in a mesh: py: 2 (over y), px: 4 (over x, core), pz: 4 (over z).
Axes of the slice: x: 2, y: 2, z: 4, core: 2. Of those that a mesh axis runs over, the one named last changes fastest.
Arguments:
- tracer: float32 [32, 512, 32, 128], P('py', 'px', 'pz'), may hold values from 0.2 to 1.8
- conductance: float32 [32, 512, 32, 128], P('py', 'px', 'pz'), may hold values from 0.03 to 0.15
- source: float32 [32, 512, 32, 128], P('py', 'px', 'pz'), may hold values from -0.2 to 0.2
Outputs:
- potential: float32 [32, 512, 32, 128], P('py', 'px', 'pz')
- tracer_end: float32 [32, 512, 32, 128], P('py', 'px', 'pz')
The draws below stay inside these ranges and needn't reach their ends.
All inputs are finite; a program needn't handle non-finite values.
Results may differ from the reference program's by a relative error of at most 0.00002.
Values sent between devices are 32-bit elements; how exact they have to be, the bound alone decides.
A program may use at most 320 MiB of HBM per device.

```python
import jax
import jax.numpy as jnp
from jax import lax

GRID_Y = 32
GRID_X = 512
GRID_Z = 32
MEMBERS = 128
STEPS = 4


def block_scale(stream_key, shape, shards, least, high):
    factor_of = 1.0
    for position, parts in shards:
        draws = jax.random.uniform(jax.random.fold_in(jax.random.fold_in(stream_key, 6), position), (parts,), jnp.float32, least / len(shards), high / len(shards))
        factor_of = factor_of * jnp.repeat(jnp.exp(draws), shape[position] // parts).reshape((-1,) + (1,) * (len(shape) - 1 - position))
    return factor_of


def setup_inputs(seed: int = 0) -> dict:
    splits = jax.random.split(jax.random.key(seed), 4)
    tracer = jnp.clip(0.2 + 1.5999999 * jax.random.uniform(splits[0], (GRID_Y, GRID_X, GRID_Z, MEMBERS), jnp.float32) ** block_scale(splits[0], (GRID_Y, GRID_X, GRID_Z, MEMBERS), ((0, 2), (1, 4), (2, 4)), -0.2, 0.2), 0.2, 1.8)
    conductance = jnp.clip(0.03 + 0.120000007 * jax.random.uniform(splits[1], (GRID_Y, GRID_X, GRID_Z, MEMBERS), jnp.float32) ** block_scale(splits[1], (GRID_Y, GRID_X, GRID_Z, MEMBERS), ((0, 2), (1, 4), (2, 4)), -0.2, 0.2), 0.03, 0.15)
    source = jnp.clip(jax.random.uniform(splits[2], (GRID_Y, GRID_X, GRID_Z, MEMBERS), jnp.float32, -0.2, 0.2) * block_scale(splits[2], (GRID_Y, GRID_X, GRID_Z, MEMBERS), ((0, 2), (1, 4), (2, 4)), -0.4, 0.0), -0.2, 0.2)
    return dict(tracer=tracer, conductance=conductance, source=source)


def strip_edges(values, dims):
    for dim in dims:
        values = lax.slice_in_dim(values, 1, values.shape[dim] - 1, axis=dim)
    return values


def neighbour(values, dim, start, dims):
    others = [other for other in dims if other != dim]
    values = strip_edges(values, others)
    return lax.slice_in_dim(values, start, start + values.shape[dim] - 2, axis=dim)


def one_step(padded, conductance, source):
    middle = strip_edges(padded, (0, 1, 2))
    lower = [neighbour(padded, dim, 0, (0, 1, 2)) for dim in (0, 1, 2)]
    upper = [neighbour(padded, dim, 2, (0, 1, 2)) for dim in (0, 1, 2)]
    spread = lower[0] + upper[0] + lower[1] + upper[1] + lower[2] + upper[2] - 6.0 * middle
    return middle + conductance * spread + source


def reference(tracer, conductance, source):
    for step in range(STEPS):
        tracer = one_step(jnp.pad(tracer, ((1, 1), (1, 1), (1, 1), (0, 0)), mode="wrap"), conductance, source)
    potential = jnp.cumsum(tracer, axis=2) / GRID_Z
    return potential, tracer
```

```python
import functools

import jax
import jax.numpy as jnp
from jax import lax
from jax.experimental import pallas as pl
from jax.experimental.pallas import tpu as pltpu
from jax.sharding import PartitionSpec as P

STEPS = 4
MESH = pl.DeviceIdType.MESH


def chunks_of(cells):
    for parts in (8, 4, 2):
        if cells % (8 * parts) == 0:
            return parts
    raise ValueError("x extent")


def evolve(
    counts, parts, deep, tracer, conductance, source, end, below,
    field, coeff, gain, zhalo, yhalo, xhalo, zface, entering, leaving,
    load_sem, zsend, zrecv, ysend, yrecv, xsend, xrecv, psend, precv, store_sem,
):
    rows_y, all_rows, members = tracer.shape
    cells = all_rows // deep
    wide = cells // parts
    rows = wide * deep
    count = dict(zip(("py", "px", "pz"), counts))
    mine = {axis: lax.axis_index(axis) for axis in count}
    after = {axis: lax.rem(mine[axis] + 1, count[axis]) for axis in count}
    before = {axis: lax.rem(mine[axis] + count[axis] - 1, count[axis]) for axis in count}
    body_y = pl.ds(1, rows_y)

    def span(c):
        return pl.ds(pl.multiple_of(c * rows, 8), rows)

    def inner(c):
        return pl.ds(pl.multiple_of(c * rows + deep, 8), rows)

    def cell_span(c):
        return pl.ds(pl.multiple_of(c * wide, 8), wide)

    def load(which, c):
        hbm, dst = (
            (tracer, field.at[0, body_y, inner(c), :]),
            (conductance, coeff.at[:, span(c), :]),
            (source, gain.at[:, span(c), :]),
        )[which]
        return pltpu.make_async_copy(hbm.at[:, span(c), :], dst, load_sem.at[which, c])

    def remote(src, dst, send, recv, axis, target):
        return pltpu.make_async_remote_copy(
            src_ref=src, dst_ref=dst, send_sem=send, recv_sem=recv,
            device_id={axis: target}, device_id_type=MESH,
        )

    def z_copy(t, side, c):
        return remote(
            zface.at[lax.rem(t, 2), side, :, cell_span(c), :],
            zhalo.at[t, side, :, cell_span(c), :],
            zsend.at[t, side, c], zrecv.at[t, side, c],
            "pz", (after, before)[side]["pz"],
        )

    def y_copy(t, side, c):
        return remote(
            field.at[lax.rem(t, 2), (rows_y, 1)[side], inner(c), :],
            yhalo.at[t, side, span(c), :],
            ysend.at[t, side, c], yrecv.at[t, side, c],
            "py", (after, before)[side]["py"],
        )

    def x_copy(t, side):
        return remote(
            field.at[lax.rem(t, 2), body_y, pl.ds((all_rows, deep)[side], deep), :],
            xhalo.at[t, side],
            xsend.at[t, side], xrecv.at[t, side],
            "px", (after, before)[side]["px"],
        )

    def prefix_copy(c):
        return remote(
            leaving.at[:, cell_span(c), :], entering.at[:, cell_span(c), :],
            psend.at[c], precv.at[c], "pz", after["pz"],
        )

    def store_end(c):
        return pltpu.make_async_copy(
            field.at[STEPS % 2, body_y, inner(c), :], end.at[:, span(c), :], store_sem.at[0, c]
        )

    def store_below(c):
        return pltpu.make_async_copy(
            entering.at[:, cell_span(c), :], below.at[:, cell_span(c), :], store_sem.at[1, c]
        )

    def send_faces(t, c):
        for side in (0, 1):
            z_copy(t, side, c).start()
            y_copy(t, side, c).start()

        @pl.when(c == 0)
        def _():
            x_copy(t, 1).start()

        @pl.when(c == parts - 1)
        def _():
            x_copy(t, 0).start()

    def face_of(p, y, c, z):
        return field[p, y, pl.ds(c * rows + deep + z, wide, stride=deep), :]

    def keep_z_faces(p, y, c):
        zface[p, 0, y, cell_span(c), :] = face_of(p, y + 1, c, deep - 1)
        zface[p, 1, y, cell_span(c), :] = face_of(p, y + 1, c, 0)

    def each_chunk(work):
        def run(c, carry):
            work(c)
            return carry

        lax.fori_loop(0, parts, run, 0)

    each_chunk(lambda c: load(0, c).start())

    def load_rest(c):
        load(1, c).start()
        load(2, c).start()

    each_chunk(load_rest)

    barrier = pltpu.get_barrier_semaphore()
    for axis in count:
        for target in (after[axis], before[axis]):
            pl.semaphore_signal(barrier, inc=1, device_id={axis: target}, device_id_type=MESH)
    pl.semaphore_wait(barrier, 6)

    def first_faces(c):
        load(0, c).wait()

        def row(y, carry):
            keep_z_faces(0, y, c)
            return carry

        lax.fori_loop(0, rows_y, row, 0)
        send_faces(0, c)

    each_chunk(first_faces)

    def wait_sent(t, c):
        for side in (0, 1):
            z_copy(t, side, c).wait_send()
            y_copy(t, side, c).wait_send()

        @pl.when(c == 0)
        def _():
            x_copy(t, 1).wait_send()

        @pl.when(c == parts - 1)
        def _():
            x_copy(t, 0).wait_send()

    level = lax.broadcasted_iota(jnp.int32, (wide, deep, members), 1)

    def step(t, carry):
        old, new = lax.rem(t, 2), lax.rem(t + 1, 2)

        def chunk(c):
            @pl.when(t == 0)
            def _():
                load(1, c).wait()
                load(2, c).wait()

            @pl.when(t > 0)
            def _():
                wait_sent(t - 1, c)

            for side in (0, 1):
                z_copy(t, side, c).wait_recv()
                y_copy(t, side, c).wait_recv()
                field[old, (0, rows_y + 1)[side], inner(c), :] = yhalo[t, side, span(c), :]

            @pl.when(c == 0)
            def _():
                x_copy(t, 0).wait_recv()
                field[old, body_y, pl.ds(0, deep), :] = xhalo[t, 0]

            @pl.when(c == parts - 1)
            def _():
                x_copy(t, 1).wait_recv()
                field[old, body_y, pl.ds(all_rows + deep, deep), :] = xhalo[t, 1]

            def row(y, carry):
                def at(dy, dx):
                    start = pl.multiple_of(c * rows + deep + dx * deep, 8)
                    return field[old, y + 1 + dy, pl.ds(start, rows), :]

                def tall(values):
                    return jnp.broadcast_to(values[:, None, :], (wide, deep, members))

                middle = at(0, 0)
                block = middle.reshape(wide, deep, members)
                first = tall(zhalo[t, 0, y, cell_span(c), :])
                last = tall(zhalo[t, 1, y, cell_span(c), :])
                lower = jnp.where(level == 0, first, pltpu.roll(block, 1, 1))
                upper = jnp.where(level == deep - 1, last, pltpu.roll(block, deep - 1, 1))
                along = (lower + upper).reshape(rows, members)
                spread = at(-1, 0) + at(1, 0) + at(0, -1) + at(0, 1) + along - 6.0 * middle
                field[new, y + 1, inner(c), :] = (
                    middle + coeff[y, span(c), :] * spread + gain[y, span(c), :]
                )
                return carry

            lax.fori_loop(0, rows_y, row, 0)

            @pl.when(t < STEPS - 1)
            def _():
                def faces(y, carry):
                    keep_z_faces(new, y, c)
                    return carry

                lax.fori_loop(0, rows_y, faces, 0)
                send_faces(t + 1, c)

            @pl.when(t == STEPS - 1)
            def _():
                store_end(c).start()

                def totals(y, carry):
                    total = face_of(new, y + 1, c, 0)
                    for z in range(1, deep):
                        total = total + face_of(new, y + 1, c, z)
                    leaving[y, cell_span(c), :] = total
                    return carry

                lax.fori_loop(0, rows_y, totals, 0)

                @pl.when(mine["pz"] == 0)
                def _():
                    entering[:, cell_span(c), :] = jnp.zeros((rows_y, wide, members), jnp.float32)

                @pl.when(mine["pz"] > 0)
                def _():
                    prefix_copy(c).wait_recv()
                    leaving[:, cell_span(c), :] += entering[:, cell_span(c), :]

                @pl.when(mine["pz"] < count["pz"] - 1)
                def _():
                    prefix_copy(c).start()

                store_below(c).start()

        each_chunk(chunk)
        return carry

    lax.fori_loop(0, STEPS, step, 0)

    def finish(c):
        wait_sent(STEPS - 1, c)
        store_end(c).wait()
        store_below(c).wait()

        @pl.when(mine["pz"] < count["pz"] - 1)
        def _():
            prefix_copy(c).wait_send()

    each_chunk(finish)


def sums(depth, end, below, potential, tracer_end):
    _, all_rows, members = end.shape
    cells = below.shape[1]
    deep = all_rows // cells
    values = end[0]
    tracer_end[0] = values
    block = values.reshape(cells, deep, members)
    level = lax.broadcasted_iota(jnp.int32, block.shape, 1)
    reach = 1
    while reach < deep:
        block = block + jnp.where(level >= reach, pltpu.roll(block, reach, 1), 0.0)
        reach *= 2
    block = block + jnp.broadcast_to(below[0][:, None, :], block.shape)
    potential[0] = (block / depth).reshape(all_rows, members)


def on_device(counts, tracer, conductance, source):
    shape = tracer.shape
    rows_y, cells, deep, members = shape
    parts = chunks_of(cells)
    rows = cells * deep
    flat = (rows_y, rows, members)
    anywhere = pl.BlockSpec(memory_space=pl.ANY)
    f32 = jnp.float32
    dma = pltpu.SemaphoreType.DMA
    end, below = pl.pallas_call(
        functools.partial(evolve, counts, parts, deep),
        out_shape=(
            jax.ShapeDtypeStruct(flat, f32),
            jax.ShapeDtypeStruct((rows_y, cells, members), f32),
        ),
        in_specs=[anywhere] * 3,
        out_specs=(anywhere, anywhere),
        scratch_shapes=[
            pltpu.VMEM((2, rows_y + 2, rows + 2 * deep, members), f32),
            pltpu.VMEM(flat, f32),
            pltpu.VMEM(flat, f32),
            pltpu.VMEM((STEPS, 2, rows_y, cells, members), f32),
            pltpu.VMEM((STEPS, 2, rows, members), f32),
            pltpu.VMEM((STEPS, 2, rows_y, deep, members), f32),
            pltpu.VMEM((2, 2, rows_y, cells, members), f32),
            pltpu.VMEM((rows_y, cells, members), f32),
            pltpu.VMEM((rows_y, cells, members), f32),
            dma((3, parts)),
            dma((STEPS, 2, parts)), dma((STEPS, 2, parts)),
            dma((STEPS, 2, parts)), dma((STEPS, 2, parts)),
            dma((STEPS, 2)), dma((STEPS, 2)),
            dma((parts,)), dma((parts,)),
            dma((2, parts)),
        ],
        compiler_params=pltpu.CompilerParams(
            collective_id=0, has_side_effects=True, vmem_limit_bytes=64 * 1000 * 1000
        ),
        name="evolve",
    )(*(array.reshape(flat) for array in (tracer, conductance, source)))
    tall = pl.BlockSpec((1, rows, members), lambda y: (y, 0, 0))
    potential, tracer_end = pl.pallas_call(
        functools.partial(sums, deep * counts[2]),
        grid=(rows_y,),
        out_shape=(jax.ShapeDtypeStruct(flat, f32),) * 2,
        in_specs=[tall, pl.BlockSpec((1, cells, members), lambda y: (y, 0, 0))],
        out_specs=(tall, tall),
        name="sums",
    )(end, below)
    return potential.reshape(shape), tracer_end.reshape(shape)


def solution(mesh):
    placed = P("py", "px", "pz", None)
    counts = tuple(mesh.shape[axis] for axis in ("py", "px", "pz"))
    return jax.shard_map(
        functools.partial(on_device, counts),
        mesh=mesh,
        in_specs=(placed,) * 3,
        out_specs=(placed,) * 2,
        check_vma=False,
    )
```

```python
import functools

import jax
import jax.numpy as jnp
from jax import lax
from jax.experimental import pallas as pl
from jax.experimental.pallas import tpu as pltpu
from jax.sharding import PartitionSpec as P

STEPS = 4
MESH = pl.DeviceIdType.MESH


def chunks_of(cells):
    for parts in (8, 4, 2):
        if cells % (8 * parts) == 0:
            return parts
    raise ValueError("x extent")


def evolve(
    counts, parts, deep, tracer, conductance, source, end, below,
    field, coeff, gain, zhalo, yhalo, xhalo, zface, entering, leaving,
    load_sem, zsend, zrecv, ysend, yrecv, xsend, xrecv, psend, precv,
):
    rows_y, all_rows, members = tracer.shape
    cells = all_rows // deep
    wide = cells // parts
    rows = wide * deep
    halves = psend.shape[1]
    count = dict(zip(("py", "px", "pz"), counts))
    mine = {axis: lax.axis_index(axis) for axis in count}
    after = {axis: lax.rem(mine[axis] + 1, count[axis]) for axis in count}
    before = {axis: lax.rem(mine[axis] + count[axis] - 1, count[axis]) for axis in count}
    body_y = pl.ds(1, rows_y)

    def span(c):
        return pl.ds(pl.multiple_of(c * rows, 8), rows)

    def inner(c):
        return pl.ds(pl.multiple_of(c * rows + deep, 8), rows)

    def cell_span(c):
        return pl.ds(pl.multiple_of(c * wide, 8), wide)

    def load(which, c):
        hbm, dst = (
            (tracer, field.at[0, body_y, inner(c), :]),
            (conductance, coeff.at[:, span(c), :]),
            (source, gain.at[:, span(c), :]),
        )[which]
        return pltpu.make_async_copy(hbm.at[:, span(c), :], dst, load_sem.at[which, c])

    def remote(src, dst, send, recv, axis, target):
        return pltpu.make_async_remote_copy(
            src_ref=src, dst_ref=dst, send_sem=send, recv_sem=recv,
            device_id={axis: target}, device_id_type=MESH,
        )

    def z_copy(t, side, c):
        return remote(
            zface.at[lax.rem(t, 2), side, :, cell_span(c), :],
            zhalo.at[t, side, :, cell_span(c), :],
            zsend.at[t, side, c], zrecv.at[t, side, c],
            "pz", (after, before)[side]["pz"],
        )

    def y_copy(t, side, c):
        return remote(
            field.at[lax.rem(t, 2), (rows_y, 1)[side], inner(c), :],
            yhalo.at[t, side, span(c), :],
            ysend.at[t, side, c], yrecv.at[t, side, c],
            "py", (after, before)[side]["py"],
        )

    def x_copy(t, side):
        return remote(
            field.at[lax.rem(t, 2), body_y, pl.ds((all_rows, deep)[side], deep), :],
            xhalo.at[t, side],
            xsend.at[t, side], xrecv.at[t, side],
            "px", (after, before)[side]["px"],
        )

    def part_y(h):
        return pl.ds(h * (rows_y // halves), rows_y // halves)

    def prefix_copy(c, h):
        return remote(
            leaving.at[part_y(h), cell_span(c), :], entering.at[part_y(h), cell_span(c), :],
            psend.at[c, h], precv.at[c, h], "pz", after["pz"],
        )

    def send_faces(t, c):
        for side in (0, 1):
            z_copy(t, side, c).start()
            y_copy(t, side, c).start()

        @pl.when(c == 0)
        def _():
            x_copy(t, 1).start()

        @pl.when(c == parts - 1)
        def _():
            x_copy(t, 0).start()

    def face_of(p, y, c, z):
        return field[p, y, pl.ds(c * rows + deep + z, wide, stride=deep), :]

    def keep_z_faces(p, y, c):
        zface[p, 0, y, cell_span(c), :] = face_of(p, y + 1, c, deep - 1)
        zface[p, 1, y, cell_span(c), :] = face_of(p, y + 1, c, 0)

    def each_chunk(work):
        def run(c, carry):
            work(c)
            return carry

        lax.fori_loop(0, parts, run, 0)

    load(0, 0).start()
    load(0, 1).start()

    barrier = pltpu.get_barrier_semaphore()
    for axis in count:
        for target in (after[axis], before[axis]):
            pl.semaphore_signal(barrier, inc=1, device_id={axis: target}, device_id_type=MESH)
    pl.semaphore_wait(barrier, 6)

    def first_faces(c):
        load(0, c).wait()

        @pl.when(c < parts - 2)
        def _():
            load(0, c + 2).start()

        def row(y, carry):
            keep_z_faces(0, y, c)
            return carry

        lax.fori_loop(0, rows_y, row, 0)
        send_faces(0, c)
        load(1, c).start()
        load(2, c).start()

    each_chunk(first_faces)

    def wait_sent(t, c):
        for side in (0, 1):
            z_copy(t, side, c).wait_send()
            y_copy(t, side, c).wait_send()

        @pl.when(c == 0)
        def _():
            x_copy(t, 1).wait_send()

        @pl.when(c == parts - 1)
        def _():
            x_copy(t, 0).wait_send()

    level = lax.broadcasted_iota(jnp.int32, (wide, deep, members), 1)

    def step(t, carry):
        old, new = lax.rem(t, 2), lax.rem(t + 1, 2)

        def chunk(c):
            @pl.when(t == 0)
            def _():
                load(1, c).wait()
                load(2, c).wait()

            @pl.when(t > 0)
            def _():
                wait_sent(t - 1, c)

            for side in (0, 1):
                z_copy(t, side, c).wait_recv()
                y_copy(t, side, c).wait_recv()
                field[old, (0, rows_y + 1)[side], inner(c), :] = yhalo[t, side, span(c), :]

            @pl.when(c == 0)
            def _():
                x_copy(t, 0).wait_recv()
                field[old, body_y, pl.ds(0, deep), :] = xhalo[t, 0]

            @pl.when(c == parts - 1)
            def _():
                x_copy(t, 1).wait_recv()
                field[old, body_y, pl.ds(all_rows + deep, deep), :] = xhalo[t, 1]

            def row(y, carry):
                def at(dy, dx):
                    start = pl.multiple_of(c * rows + deep + dx * deep, 8)
                    return field[old, y + 1 + dy, pl.ds(start, rows), :]

                def tall(values):
                    return jnp.broadcast_to(values[:, None, :], (wide, deep, members))

                middle = at(0, 0)
                block = middle.reshape(wide, deep, members)
                first = tall(zhalo[t, 0, y, cell_span(c), :])
                last = tall(zhalo[t, 1, y, cell_span(c), :])
                lower = jnp.where(level == 0, first, pltpu.roll(block, 1, 1))
                upper = jnp.where(level == deep - 1, last, pltpu.roll(block, deep - 1, 1))
                along = (lower + upper).reshape(rows, members)
                spread = at(-1, 0) + at(1, 0) + at(0, -1) + at(0, 1) + along - 6.0 * middle
                field[new, y + 1, inner(c), :] = (
                    middle + coeff[y, span(c), :] * spread + gain[y, span(c), :]
                )
                return carry

            lax.fori_loop(0, rows_y, row, 0)

            @pl.when(t < STEPS - 1)
            def _():
                def faces(y, carry):
                    keep_z_faces(new, y, c)
                    return carry

                lax.fori_loop(0, rows_y, faces, 0)
                send_faces(t + 1, c)

            @pl.when(t == STEPS - 1)
            def _():
                def totals(y, carry):
                    end[y, span(c), :] = field[new, y + 1, inner(c), :]
                    total = face_of(new, y + 1, c, 0)
                    for z in range(1, deep):
                        total = total + face_of(new, y + 1, c, z)
                    leaving[y, cell_span(c), :] = total
                    return carry

                lax.fori_loop(0, rows_y, totals, 0)

                @pl.when(mine["pz"] == 0)
                def _():
                    entering[:, cell_span(c), :] = jnp.zeros((rows_y, wide, members), jnp.float32)
                    for h in range(halves):
                        prefix_copy(c, h).start()

        each_chunk(chunk)
        return carry

    lax.fori_loop(0, STEPS, step, 0)

    @pl.when(mine["pz"] > 0)
    def _():
        def pass_on(c):
            for h in range(halves):
                prefix_copy(c, h).wait_recv()

                @pl.when(mine["pz"] < count["pz"] - 1)
                def _():
                    leaving[part_y(h), cell_span(c), :] += entering[part_y(h), cell_span(c), :]
                    prefix_copy(c, h).start()

        each_chunk(pass_on)

    def keep_below(y, carry):
        below[y] = entering[y]
        return carry

    lax.fori_loop(0, rows_y, keep_below, 0)

    def finish(c):
        wait_sent(STEPS - 1, c)

        @pl.when(mine["pz"] < count["pz"] - 1)
        def _():
            for h in range(halves):
                prefix_copy(c, h).wait_send()

    each_chunk(finish)


def sums(depth, end, below, potential, tracer_end, ready, end_sem, sum_sem):
    rows_y, all_rows, members = end.shape
    cells = below.shape[1]
    deep = all_rows // cells
    slots = ready.shape[0]
    level = lax.broadcasted_iota(jnp.int32, (cells, deep, members), 1)
    whole = pltpu.make_async_copy(end, tracer_end, end_sem)
    whole.start()

    def store(y):
        slot = lax.rem(y, slots)
        return pltpu.make_async_copy(ready.at[slot], potential.at[y], sum_sem.at[slot])

    def row(y, carry):
        @pl.when(y >= slots)
        def _():
            store(y - slots).wait()

        block = end[y].reshape(cells, deep, members)
        reach = 1
        while reach < deep:
            block = block + jnp.where(level >= reach, pltpu.roll(block, reach, 1), 0.0)
            reach *= 2
        block = block + jnp.broadcast_to(below[y][:, None, :], block.shape)
        ready[lax.rem(y, slots)] = (block / depth).reshape(all_rows, members)
        store(y).start()
        return carry

    lax.fori_loop(0, rows_y, row, 0)

    def drain(y, carry):
        store(y).wait()
        return carry

    lax.fori_loop(rows_y - slots, rows_y, drain, 0)
    whole.wait()


def on_device(counts, tracer, conductance, source):
    shape = tracer.shape
    rows_y, cells, deep, members = shape
    parts = chunks_of(cells)
    rows = cells * deep
    halves = 2 if rows_y % 2 == 0 else 1
    flat = (rows_y, rows, members)
    anywhere = pl.BlockSpec(memory_space=pl.ANY)
    near = pl.BlockSpec(memory_space=pltpu.VMEM)
    f32 = jnp.float32
    dma = pltpu.SemaphoreType.DMA
    end, below = pl.pallas_call(
        functools.partial(evolve, counts, parts, deep),
        out_shape=(
            pltpu.VMEM(flat, f32),
            pltpu.VMEM((rows_y, cells, members), f32),
        ),
        in_specs=[anywhere] * 3,
        out_specs=(near, near),
        scratch_shapes=[
            pltpu.VMEM((2, rows_y + 2, rows + 2 * deep, members), f32),
            pltpu.VMEM(flat, f32),
            pltpu.VMEM(flat, f32),
            pltpu.VMEM((STEPS, 2, rows_y, cells, members), f32),
            pltpu.VMEM((STEPS, 2, rows, members), f32),
            pltpu.VMEM((STEPS, 2, rows_y, deep, members), f32),
            pltpu.VMEM((2, 2, rows_y, cells, members), f32),
            pltpu.VMEM((rows_y, cells, members), f32),
            pltpu.VMEM((rows_y, cells, members), f32),
            dma((3, parts)),
            dma((STEPS, 2, parts)), dma((STEPS, 2, parts)),
            dma((STEPS, 2, parts)), dma((STEPS, 2, parts)),
            dma((STEPS, 2)), dma((STEPS, 2)),
            dma((parts, halves)), dma((parts, halves)),
        ],
        compiler_params=pltpu.CompilerParams(
            collective_id=0, has_side_effects=True, vmem_limit_bytes=53 * 1024 * 1024 + 524288
        ),
        name="evolve",
    )(*(array.reshape(flat) for array in (tracer, conductance, source)))
    slots = min(4, rows_y)
    potential, tracer_end = pl.pallas_call(
        functools.partial(sums, deep * counts[2]),
        out_shape=(jax.ShapeDtypeStruct(flat, f32),) * 2,
        in_specs=[near, near],
        out_specs=(anywhere, anywhere),
        scratch_shapes=[pltpu.VMEM((slots, rows, members), f32), dma(()), dma((slots,))],
        compiler_params=pltpu.CompilerParams(vmem_limit_bytes=16 * 1024 * 1024),
        name="sums",
    )(end, below)
    return potential.reshape(shape), tracer_end.reshape(shape)


def solution(mesh):
    placed = P("py", "px", "pz", None)
    counts = tuple(mesh.shape[axis] for axis in ("py", "px", "pz"))
    return jax.shard_map(
        functools.partial(on_device, counts),
        mesh=mesh,
        in_specs=(placed,) * 3,
        out_specs=(placed,) * 2,
        check_vma=False,
    )
```

```python
import functools

import jax
import jax.numpy as jnp
from jax import lax
from jax.experimental import pallas as pl
from jax.experimental.pallas import tpu as pltpu
from jax.sharding import PartitionSpec as P

STEPS = 4
MESH = pl.DeviceIdType.MESH


def chunks_of(cells):
    for parts in (8, 4, 2):
        if cells % (8 * parts) == 0:
            return parts
    raise ValueError("x extent")


def evolve(
    counts, parts, deep, tracer, conductance, source, end, below,
    field, coeff, gain, zhalo, yhalo, xhalo, zface, entering, leaving,
    load_sem, zsend, zrecv, ysend, yrecv, xsend, xrecv, psend, precv,
):
    rows_y, all_rows, members = tracer.shape
    cells = all_rows // deep
    wide = cells // parts
    rows = wide * deep
    halves = psend.shape[1]
    count = dict(zip(("py", "px", "pz"), counts))
    mine = {axis: lax.axis_index(axis) for axis in count}
    after = {axis: lax.rem(mine[axis] + 1, count[axis]) for axis in count}
    before = {axis: lax.rem(mine[axis] + count[axis] - 1, count[axis]) for axis in count}
    body_y = pl.ds(1, rows_y)

    def span(c):
        return pl.ds(pl.multiple_of(c * rows, 8), rows)

    def inner(c):
        return pl.ds(pl.multiple_of(c * rows + deep, 8), rows)

    def cell_span(c):
        return pl.ds(pl.multiple_of(c * wide, 8), wide)

    def load(which, c):
        hbm, dst = (
            (tracer, field.at[0, body_y, inner(c), :]),
            (conductance, coeff.at[:, span(c), :]),
            (source, gain.at[:, span(c), :]),
        )[which]
        return pltpu.make_async_copy(hbm.at[:, span(c), :], dst, load_sem.at[which, c])

    def remote(src, dst, send, recv, axis, target):
        return pltpu.make_async_remote_copy(
            src_ref=src, dst_ref=dst, send_sem=send, recv_sem=recv,
            device_id={axis: target}, device_id_type=MESH,
        )

    def z_copy(t, side, c):
        return remote(
            zface.at[lax.rem(t, 2), side, :, cell_span(c), :],
            zhalo.at[t, side, :, cell_span(c), :],
            zsend.at[t, side, c], zrecv.at[t, side, c],
            "pz", (after, before)[side]["pz"],
        )

    def y_copy(t, side, c):
        return remote(
            field.at[lax.rem(t, 2), (rows_y, 1)[side], inner(c), :],
            yhalo.at[t, side, span(c), :],
            ysend.at[t, side, c], yrecv.at[t, side, c],
            "py", (after, before)[side]["py"],
        )

    def x_copy(t, side):
        return remote(
            field.at[lax.rem(t, 2), body_y, pl.ds((all_rows, deep)[side], deep), :],
            xhalo.at[t, side],
            xsend.at[t, side], xrecv.at[t, side],
            "px", (after, before)[side]["px"],
        )

    def part_y(h):
        return pl.ds(h * (rows_y // halves), rows_y // halves)

    def prefix_copy(c, h):
        return remote(
            leaving.at[part_y(h), cell_span(c), :], entering.at[part_y(h), cell_span(c), :],
            psend.at[c, h], precv.at[c, h], "pz", after["pz"],
        )

    def send_faces(t, c):
        for side in (0, 1):
            z_copy(t, side, c).start()
            y_copy(t, side, c).start()

        @pl.when(c == 0)
        def _():
            x_copy(t, 1).start()

        @pl.when(c == parts - 1)
        def _():
            x_copy(t, 0).start()

    def face_of(p, y, c, z):
        return field[p, y, pl.ds(c * rows + deep + z, wide, stride=deep), :]

    def keep_z_faces(p, y, c):
        zface[p, 0, y, cell_span(c), :] = face_of(p, y + 1, c, deep - 1)
        zface[p, 1, y, cell_span(c), :] = face_of(p, y + 1, c, 0)

    def each_chunk(work):
        def run(c, carry):
            work(c)
            return carry

        lax.fori_loop(0, parts, run, 0)

    load(0, 0).start()
    load(0, 1).start()

    barrier = pltpu.get_barrier_semaphore()
    for axis in count:
        for target in (after[axis], before[axis]):
            pl.semaphore_signal(barrier, inc=1, device_id={axis: target}, device_id_type=MESH)
    pl.semaphore_wait(barrier, 6)

    def first_faces(c):
        load(0, c).wait()

        @pl.when(c < parts - 2)
        def _():
            load(0, c + 2).start()

        def row(y, carry):
            keep_z_faces(0, y, c)
            return carry

        lax.fori_loop(0, rows_y, row, 0)
        send_faces(0, c)
        load(1, c).start()
        load(2, c).start()

    each_chunk(first_faces)

    def wait_sent(t, c):
        for side in (0, 1):
            z_copy(t, side, c).wait_send()
            y_copy(t, side, c).wait_send()

        @pl.when(c == 0)
        def _():
            x_copy(t, 1).wait_send()

        @pl.when(c == parts - 1)
        def _():
            x_copy(t, 0).wait_send()

    level = lax.broadcasted_iota(jnp.int32, (wide, deep, members), 1)

    def step(t, carry):
        old, new = lax.rem(t, 2), lax.rem(t + 1, 2)

        def chunk(c):
            @pl.when(t == 0)
            def _():
                load(1, c).wait()
                load(2, c).wait()

            @pl.when(t > 0)
            def _():
                wait_sent(t - 1, c)

            for side in (0, 1):
                z_copy(t, side, c).wait_recv()
                y_copy(t, side, c).wait_recv()
                field[old, (0, rows_y + 1)[side], inner(c), :] = yhalo[t, side, span(c), :]

            @pl.when(c == 0)
            def _():
                x_copy(t, 0).wait_recv()
                field[old, body_y, pl.ds(0, deep), :] = xhalo[t, 0]

            @pl.when(c == parts - 1)
            def _():
                x_copy(t, 1).wait_recv()
                field[old, body_y, pl.ds(all_rows + deep, deep), :] = xhalo[t, 1]

            def row(y, carry):
                def at(dy, dx):
                    start = pl.multiple_of(c * rows + deep + dx * deep, 8)
                    return field[old, y + 1 + dy, pl.ds(start, rows), :]

                def tall(values):
                    return jnp.broadcast_to(values[:, None, :], (wide, deep, members))

                middle = at(0, 0)
                block = middle.reshape(wide, deep, members)
                first = tall(zhalo[t, 0, y, cell_span(c), :])
                last = tall(zhalo[t, 1, y, cell_span(c), :])
                lower = jnp.where(level == 0, first, pltpu.roll(block, 1, 1))
                upper = jnp.where(level == deep - 1, last, pltpu.roll(block, deep - 1, 1))
                along = (lower + upper).reshape(rows, members)
                spread = at(-1, 0) + at(1, 0) + at(0, -1) + at(0, 1) + along - 6.0 * middle
                field[new, y + 1, inner(c), :] = (
                    middle + coeff[y, span(c), :] * spread + gain[y, span(c), :]
                )
                return carry

            lax.fori_loop(0, rows_y, row, 0)

            @pl.when(t < STEPS - 1)
            def _():
                def faces(y, carry):
                    keep_z_faces(new, y, c)
                    return carry

                lax.fori_loop(0, rows_y, faces, 0)
                send_faces(t + 1, c)

            @pl.when(t == STEPS - 1)
            def _():
                def totals(y, carry):
                    end[y, span(c), :] = field[new, y + 1, inner(c), :]
                    total = face_of(new, y + 1, c, 0)
                    for z in range(1, deep):
                        total = total + face_of(new, y + 1, c, z)
                    leaving[y, cell_span(c), :] = total
                    return carry

                lax.fori_loop(0, rows_y, totals, 0)

                @pl.when(mine["pz"] == 0)
                def _():
                    entering[:, cell_span(c), :] = jnp.zeros((rows_y, wide, members), jnp.float32)
                    for h in range(halves):
                        prefix_copy(c, h).start()

        each_chunk(chunk)
        return carry

    lax.fori_loop(0, STEPS, step, 0)

    @pl.when(mine["pz"] > 0)
    def _():
        def pass_on(c):
            for h in range(halves):
                prefix_copy(c, h).wait_recv()

                @pl.when(mine["pz"] < count["pz"] - 1)
                def _():
                    leaving[part_y(h), cell_span(c), :] += entering[part_y(h), cell_span(c), :]
                    prefix_copy(c, h).start()

        each_chunk(pass_on)

    def keep_below(y, carry):
        below[y] = entering[y]
        return carry

    lax.fori_loop(0, rows_y, keep_below, 0)

    def finish(c):
        wait_sent(STEPS - 1, c)

        @pl.when(mine["pz"] < count["pz"] - 1)
        def _():
            for h in range(halves):
                prefix_copy(c, h).wait_send()

    each_chunk(finish)


def sums(depth, end, below, potential, tracer_end, ready, end_sem, sum_sem):
    rows_y, all_rows, members = end.shape
    cells = below.shape[1]
    deep = all_rows // cells
    slots = ready.shape[0]
    level = lax.broadcasted_iota(jnp.int32, (cells, deep, members), 1)
    whole = pltpu.make_async_copy(end, tracer_end, end_sem)
    whole.start()

    def store(y):
        slot = lax.rem(y, slots)
        return pltpu.make_async_copy(ready.at[slot], potential.at[y], sum_sem.at[slot])

    def row(y, carry):
        @pl.when(y >= slots)
        def _():
            store(y - slots).wait()

        block = end[y].reshape(cells, deep, members)
        reach = 1
        while reach < deep:
            block = block + jnp.where(level >= reach, pltpu.roll(block, reach, 1), 0.0)
            reach *= 2
        block = block + jnp.broadcast_to(below[y][:, None, :], block.shape)
        ready[lax.rem(y, slots)] = (block / depth).reshape(all_rows, members)
        store(y).start()
        return carry

    lax.fori_loop(0, rows_y, row, 0)

    def drain(y, carry):
        store(y).wait()
        return carry

    lax.fori_loop(rows_y - slots, rows_y, drain, 0)
    whole.wait()


def on_device(counts, tracer, conductance, source):
    shape = tracer.shape
    rows_y, cells, deep, members = shape
    parts = chunks_of(cells)
    rows = cells * deep
    halves = next((h for h in (4, 2) if rows_y % h == 0), 1)
    flat = (rows_y, rows, members)
    anywhere = pl.BlockSpec(memory_space=pl.ANY)
    near = pl.BlockSpec(memory_space=pltpu.VMEM)
    f32 = jnp.float32
    dma = pltpu.SemaphoreType.DMA
    end, below = pl.pallas_call(
        functools.partial(evolve, counts, parts, deep),
        out_shape=(
            pltpu.VMEM(flat, f32),
            pltpu.VMEM((rows_y, cells, members), f32),
        ),
        in_specs=[anywhere] * 3,
        out_specs=(near, near),
        scratch_shapes=[
            pltpu.VMEM((2, rows_y + 2, rows + 2 * deep, members), f32),
            pltpu.VMEM(flat, f32),
            pltpu.VMEM(flat, f32),
            pltpu.VMEM((STEPS, 2, rows_y, cells, members), f32),
            pltpu.VMEM((STEPS, 2, rows, members), f32),
            pltpu.VMEM((STEPS, 2, rows_y, deep, members), f32),
            pltpu.VMEM((2, 2, rows_y, cells, members), f32),
            pltpu.VMEM((rows_y, cells, members), f32),
            pltpu.VMEM((rows_y, cells, members), f32),
            dma((3, parts)),
            dma((STEPS, 2, parts)), dma((STEPS, 2, parts)),
            dma((STEPS, 2, parts)), dma((STEPS, 2, parts)),
            dma((STEPS, 2)), dma((STEPS, 2)),
            dma((parts, halves)), dma((parts, halves)),
        ],
        compiler_params=pltpu.CompilerParams(
            collective_id=0, has_side_effects=True, vmem_limit_bytes=53 * 1024 * 1024 + 524288
        ),
        name="evolve",
    )(*(array.reshape(flat) for array in (tracer, conductance, source)))
    slots = min(4, rows_y)
    potential, tracer_end = pl.pallas_call(
        functools.partial(sums, deep * counts[2]),
        out_shape=(jax.ShapeDtypeStruct(flat, f32),) * 2,
        in_specs=[near, near],
        out_specs=(anywhere, anywhere),
        scratch_shapes=[pltpu.VMEM((slots, rows, members), f32), dma(()), dma((slots,))],
        compiler_params=pltpu.CompilerParams(vmem_limit_bytes=16 * 1024 * 1024),
        name="sums",
    )(end, below)
    return potential.reshape(shape), tracer_end.reshape(shape)


def solution(mesh):
    placed = P("py", "px", "pz", None)
    counts = tuple(mesh.shape[axis] for axis in ("py", "px", "pz"))
    return jax.shard_map(
        functools.partial(on_device, counts),
        mesh=mesh,
        in_specs=(placed,) * 3,
        out_specs=(placed,) * 2,
        check_vma=False,
    )
```
